32 devices in a mesh: groups: 2 (over x), blk: 16 (over z, y, core).
Axes of the slice: x: 2, y: 2, z: 4, core: 2. Of those that a mesh axis runs over, the one named last changes fastest.
Arguments:
- embeddings: bfloat16 [12288, 512], P(('groups', 'blk')), parts along dimension 0, may hold values from -24 to 24
- cluster_ids: int32 [12288], P(('groups', 'blk')), parts along dimension 0, may hold values from 0 to 63, as said below
- cluster_sizes: int32 [128], P('groups'), parts along dimension 0, may hold values from 12 to 960, as said below
Outputs:
- log_density: float32 [12288], P(('groups', 'blk')), parts along dimension 0
- centrality: float32 [12288], P(('groups', 'blk')), parts along dimension 0
The draws below stay inside these ranges and needn't reach their ends.
There are 2 independent parts, one for each index of `groups`. The reference program is written for one: setup_inputs(seed, part) draws one part's arguments, and reference() takes and returns one part's arrays. A program takes and returns all parts, laid end to end along the dimension named above; each array names one. Nothing has to cross between parts.
Inputs may be any that keep to these rules, and one draw needn't show every extreme that they name: cluster_sizes[c] is the number of rows whose cluster id is c; the sizes sum to 6144 and the largest is exactly 960. `cluster_ids`: rows are dealt to the devices of blk: with n the number of devices of blk and E_c the sum of cluster_sizes[c'] mod n over the clusters c' < c, device s holds cluster_sizes[c] // n rows of cluster c, plus one more exactly when (s - E_c) mod n < cluster_sizes[c] mod n. Within a device the rows stand in no particular order.
All inputs are finite; a program needn't handle non-finite values.
Results may differ from the reference program's by a relative error of at most 0.00065.
The reference program's roundings to bfloat16 on the way (of `unit`) count: a program that leaves them out, or rounds other values in their place, can miss the bound.
Values may be sent and summed in bfloat16 or wider, within the bound.
No kernel may reach another device: no remote copies, remote signals or barrier semaphores. Data moves between devices by JAX's collectives and lax.ppermute only.
A program may use at most 64 MiB of HBM per device.

```python
import math
import jax
import jax.numpy as jnp
from jax import lax

D = 512
CLUSTERS = 64
ROWS = 6144
MOST = 960
N_BLK = 16


def window_layout(key):
    layout_key = jax.random.fold_in(key, 11)
    cut_key, perm_key, shuffle_key = jax.random.split(layout_key, 3)
    largest = ROWS * 5 // 32
    fewest = ROWS // 512
    leftover = ROWS - largest - (CLUSTERS - 1) * fewest
    stride = largest - fewest
    fixed_cuts = leftover // stride
    uneven_boundaries = CLUSTERS - 2 - fixed_cuts
    grid_cuts = jnp.arange(1, fixed_cuts + 1, dtype=jnp.int32) * stride
    random_cuts = jax.random.randint(cut_key, (uneven_boundaries,), 0, leftover + 1, dtype=jnp.int32)
    cuts = jnp.sort(jnp.concatenate([grid_cuts, random_cuts]))
    edges = jnp.concatenate([jnp.zeros((1,), jnp.int32), cuts, jnp.full((1,), leftover, jnp.int32)])
    pieces = edges[1:] - edges[:-1] + fewest
    sizes = jnp.concatenate([jnp.full((1,), largest, jnp.int32), pieces])
    sizes = sizes[jax.random.permutation(perm_key, CLUSTERS)]
    devices = N_BLK
    per_device = ROWS // devices
    base = sizes // devices
    extra = sizes % devices
    first = (jnp.cumsum(extra) - extra) % devices
    source_rows = jnp.arange(devices, dtype=jnp.int32)
    holds = base[None, :] + ((source_rows[:, None] - first[None, :]) % devices < extra[None, :]).astype(jnp.int32)
    running = jnp.cumsum(holds, axis=1)
    local = jnp.arange(per_device, dtype=jnp.int32)
    labels = jnp.sum((local[None, :, None] >= running[:, None, :]).astype(jnp.int32), axis=2)
    similarity_scores = jax.random.randint(shuffle_key, (devices, per_device), 0, per_device, dtype=jnp.int32) * per_device + local[None, :]
    shuffle = jnp.argsort(similarity_scores, axis=1)
    labels = jnp.take_along_axis(labels, shuffle, axis=1)
    return (sizes, labels.reshape(ROWS).astype(jnp.int32))


def draw_cluster_sizes(key, part):
    sizes, labels = window_layout(key)
    return sizes


def draw_cluster_ids(key, part):
    sizes, labels = window_layout(key)
    return labels


def draw_embeddings(key, part):
    sizes, labels = window_layout(key)
    center_key, amp_key, noise_key = jax.random.split(jax.random.fold_in(key, 23), 3)
    centers = jax.random.truncated_normal(center_key, -4.0, 4.0, (CLUSTERS, D), jnp.float32)
    amplitude = jnp.exp(jax.random.uniform(amp_key, (ROWS, 1), jnp.float32, math.log(0.2), math.log(3.0)))
    noise = jax.random.truncated_normal(noise_key, -4.0, 4.0, (ROWS, D), jnp.float32)
    values = amplitude * centers[labels] + noise
    return values.astype(jnp.bfloat16)


def setup_inputs(seed: int = 0, part: int = 0) -> dict:
    streams_of = jax.random.split(jax.random.key(seed), 4)
    own_keys = jax.random.split(jax.random.fold_in(streams_of[3], part), 4)
    return {
        "embeddings": draw_embeddings(jax.random.fold_in(jax.random.fold_in(streams_of[3], part), 71), part),
        "cluster_ids": draw_cluster_ids(jax.random.fold_in(jax.random.fold_in(streams_of[3], part), 71), part),
        "cluster_sizes": draw_cluster_sizes(jax.random.fold_in(jax.random.fold_in(streams_of[3], part), 71), part),
    }


SOFTMAX_TEMP = 0.1
EPSILON = 1e-06

def unit_rows(embeddings):
    values = embeddings.astype(jnp.float32)
    scale = lax.rsqrt(lax.optimization_barrier(jnp.mean(values * values, axis=1, keepdims=True)) + EPSILON)
    return (values * (scale * values.shape[1] ** (-0.5))).astype(jnp.bfloat16)

def block_terms(remaining_rows, left_labels, right_rows, right_labels):
    similarity_scores = jnp.dot(remaining_rows, right_rows.T, preferred_element_type=jnp.float32)
    same_cluster = left_labels[:, None] == right_labels[None, :]
    return lax.optimization_barrier(jnp.sum(jnp.where(same_cluster, jnp.exp(similarity_scores / SOFTMAX_TEMP), 0.0), axis=1))

def lookup(table, one_hot):
    return lax.optimization_barrier(jnp.sum(jnp.where(one_hot, table[None, :], 0), axis=1))

def reference(embeddings, cluster_ids, cluster_sizes):
    unit = unit_rows(embeddings)
    order = jnp.argsort(cluster_ids, stable=True).astype(jnp.int32)
    sorted_unit = unit[order]
    sorted_labels = cluster_ids[order]
    window = min(ROWS, 512 + 2 * MOST)

    def one_block(index):
        lower = (index * 512).astype(jnp.int32)
        begin = jnp.clip(lower - MOST, 0, ROWS - window).astype(jnp.int32)
        remaining_rows = lax.dynamic_slice_in_dim(sorted_unit, lower, 512)
        left_labels = lax.dynamic_slice_in_dim(sorted_labels, lower, 512)
        right_rows = lax.dynamic_slice_in_dim(sorted_unit, begin, window)
        right_labels = lax.dynamic_slice_in_dim(sorted_labels, begin, window)
        return block_terms(remaining_rows, left_labels, right_rows, right_labels)
    sorted_density = lax.map(one_block, jnp.arange(ROWS // 512, dtype=jnp.int32)).reshape(ROWS)
    density = jnp.zeros((ROWS,), jnp.float32).at[order].set(sorted_density)
    member = cluster_ids[:, None] == jnp.arange(CLUSTERS, dtype=jnp.int32)[None, :]
    sizes_row = lookup(cluster_sizes, member).astype(jnp.float32)
    log_density = jnp.log(density / sizes_row)
    unit_wide = unit.astype(jnp.float32)
    centroid = jnp.dot(member.astype(jnp.float32).T, unit_wide, precision=lax.Precision.HIGHEST)
    projected = jnp.dot(unit_wide, centroid.T, precision=lax.Precision.HIGHEST)
    centrality = lax.optimization_barrier(jnp.sum(jnp.where(member, projected, 0.0), axis=1)) / sizes_row
    return (log_density, centrality)
```

```python
import functools

import jax
import jax.numpy as jnp
from jax import lax
from jax.experimental import pallas as pl
from jax.experimental.pallas import tpu as pltpu
from jax.sharding import PartitionSpec as P

SOFTMAX_TEMP = 0.1
EPSILON = 1e-06
LANES = 128
CORES = 2
F32 = jnp.float32
BF16 = jnp.bfloat16
FAR = 4096.0


def iota(shape, dim):
    return lax.broadcasted_iota(jnp.int32, shape, dim)


def pick(mask, values, axis):
    return jnp.sum(jnp.where(mask, values, 0.0), axis=axis, keepdims=True)


def one_hot(mask):
    return jnp.where(mask, 1.0, 0.0).astype(BF16)


def matmul(a, b):
    return jnp.dot(a, b, preferred_element_type=F32)


def bin_capacity(rows_dev, devices, clusters):
    total = rows_dev * devices
    largest, fewest = total * 5 // 32, total // 512
    bins = devices // CORES
    heaviest = -(-largest // devices)
    first = devices * (heaviest - 1) + 1
    bound = heaviest
    for k in range(bins + 1, clusters + 1):
        rest = total - first - fewest * (clusters - k)
        for weight in range(1, heaviest + 1):
            least = max(devices * (weight - 1) + 1, fewest)
            if (k - 1) * least > rest:
                break
            others = (rest - least + (devices - 1) * (k - 2)) // devices
            bound = max(bound, others // (bins - 1) + weight)
    return -(-bound // 8) * 8


def held(start, size, device, devices):
    last = jnp.floor((start + size - device + (devices - 1)) * (1.0 / devices))
    return last - jnp.floor((start - device + (devices - 1)) * (1.0 / devices))


def pack_kernel(devices, cap, emb, ids, sizes, send, place, bins_out, weights, picks):
    rows, width = emb.shape
    clusters = sizes.shape[1]
    bins = devices // CORES
    me = lax.axis_index("blk").astype(F32)
    values = emb[...].astype(F32)
    scale = lax.rsqrt(jnp.mean(values * values, axis=1, keepdims=True) + EPSILON)
    unit = (values * (scale * width ** (-0.5))).astype(BF16)

    size = sizes[...].astype(F32)
    down, across = iota((clusters, clusters), 0), iota((clusters, clusters), 1)
    size_col = pick(down == across, size, 1)
    start = pick(down < across, size_col, 0)
    weight = jnp.floor((size + (devices - 1)) * (1.0 / devices))
    weight_col = jnp.floor((size_col + (devices - 1)) * (1.0 / devices))
    key = weight * clusters - across[:1].astype(F32)
    key_col = weight_col * clusters - down[:, :1].astype(F32)
    rank = pick(key_col > key, 1.0, 0)
    ranked = rank == down.astype(F32)
    weights[...] = jnp.broadcast_to(pick(ranked, weight, 1), weights.shape) * bins

    bin_id = iota((bins, LANES), 0).astype(F32)
    load = weights[:bins, :] + bin_id
    picks[:bins, :] = bin_id
    for t in range(bins, clusters):
        least = jnp.min(load, axis=0, keepdims=True)
        picks[t : t + 1, :] = least
        load = jnp.where(load == least, load + weights[t : t + 1, :], load)
    chosen = picks[...]
    chosen = (chosen - jnp.floor(chosen * (1.0 / bins)) * bins)[:, :clusters]
    of_bin = pick(ranked, chosen, 0)
    bins_out[...] = of_bin
    of_bin_col = pick(down == across, of_bin, 1)
    hold = held(start, size, me, devices)
    offset = pick((of_bin == of_bin_col) & (across < down), hold, 1)
    base = of_bin_col * cap + offset

    member = ids[...] == iota((clusters, rows), 0)
    earlier = one_hot(iota((rows, rows), 0) < iota((rows, rows), 1))
    order = matmul(one_hot(member), earlier)
    target = pick(member, order + base, 0)
    place[...] = target
    slots = bins * cap
    put = one_hot(iota((slots, rows), 0).astype(F32) == target)
    send[...] = matmul(put, unit).astype(BF16)


def pair_sums(left, left_label, right, right_label, chunk):
    density, agreement = 0.0, 0.0
    for at in range(0, left.shape[0], chunk):
        cosine = lax.dot_general(
            left[at : at + chunk, :],
            right,
            (((1,), (1,)), ((), ())),
            preferred_element_type=F32,
        )
        same = left_label[at : at + chunk, :] == right_label
        terms = jnp.where(same, jnp.exp(cosine * (1.0 / SOFTMAX_TEMP)), 0.0)
        density = density + jnp.sum(terms, axis=0, keepdims=True)
        agreement = agreement + jnp.sum(jnp.where(same, cosine, 0.0), axis=0, keepdims=True)
    return density, agreement


def own_kernel(devices, cap, chunk, mine, sizes, bins_in, sums, label_row, label_col):
    clusters = sizes.shape[1]
    bins = devices // CORES
    slots = bins * cap
    me = lax.axis_index("blk")
    core = lax.rem(me, CORES)
    chip = ((me - core) // CORES).astype(F32)
    size = sizes[...].astype(F32)
    down, across = iota((clusters, clusters), 0), iota((clusters, clusters), 1)
    size_col = pick(down == across, size, 1)
    start = pick(down < across, size_col, 0)
    inside = bins_in[...] == chip
    inside_col = pick((down == across) & inside, 1.0, 1) > 0.0

    def row_labels(parity):
        start_col = pick(across < down, size, 1)
        source = (iota((clusters, bins), 1) * CORES + parity).astype(F32)
        hold = held(start_col, size_col, source, devices).astype(BF16)
        upto = one_hot((across <= down) & inside)
        ends = jnp.where(inside_col, matmul(upto, hold), FAR).astype(BF16)
        low = iota((bins, slots), 0) * cap
        spot = iota((bins, slots), 1)
        block = (spot >= low) & (spot < low + cap)
        slot = pick(block, (spot - low).astype(F32), 0)
        return pick(matmul(ends, one_hot(block)) <= slot, 1.0, 0)

    def col_labels(parity):
        source = (iota((bins, clusters), 0) * CORES + parity).astype(F32)
        hold = held(start, size, source, devices).astype(BF16)
        upto = one_hot((down <= across) & inside_col)
        ends = jnp.where(inside, matmul(hold, upto), FAR).astype(BF16)
        low = iota((slots, bins), 1) * cap
        spot = iota((slots, bins), 0)
        block = (spot >= low) & (spot < low + cap)
        slot = pick(block, (spot - low).astype(F32), 1)
        return pick(matmul(one_hot(block), ends) <= slot, 1.0, 1)

    label = row_labels(core)
    label_row[...] = label
    label_col[...] = jnp.broadcast_to(col_labels(CORES - 1 - core), label_col.shape)
    density, agreement = pair_sums(mine, col_labels(core), mine[...], label, chunk)
    sums[0:1, :] = density
    sums[1:2, :] = agreement


def mate_kernel(bins, cap, chunk, other, mine, sums, label_row, label_col, out):
    density, agreement = pair_sums(other, label_col[:, :1], mine[...], label_row[...], chunk)
    density = density + sums[0:1, :]
    agreement = agreement + sums[1:2, :]
    out[...] = jnp.zeros(out.shape, F32)
    for b in range(bins):
        out[b, 0:1, :cap] = density[:, b * cap : (b + 1) * cap]
        out[b, 1:2, :cap] = agreement[:, b * cap : (b + 1) * cap]


def finish_kernel(bins, cap, back, place, ids, sizes, log_density, centrality):
    rows = ids.shape[1]
    clusters = sizes.shape[1]
    size = sizes[...].astype(F32)
    size_col = pick(iota((clusters, clusters), 0) == iota((clusters, clusters), 1), size, 1)
    size_row = pick(ids[...] == iota((clusters, rows), 0), size_col, 0)
    target = place[...]
    low = (iota((bins, rows), 0) * cap).astype(F32)
    here = (target >= low) & (target < low + cap)
    slot = pick(here, target - low, 0)
    lane = one_hot(iota((LANES, rows), 0).astype(F32) == slot)

    def fetch(values):
        high = values.astype(BF16)
        left = values - high.astype(F32)
        mid = left.astype(BF16)
        low_part = (left - mid.astype(F32)).astype(BF16)
        found = (matmul(low_part, lane) + matmul(mid, lane)) + matmul(high, lane)
        return pick(here, found, 0)

    log_density[...] = jnp.log(fetch(back[:, 0, :]) / size_row)
    centrality[...] = fetch(back[:, 1, :]) / size_row


def call(kernel, out, operands, scratch=(), flops=0, name=None):
    return pl.pallas_call(
        kernel,
        out_shape=out,
        in_specs=[pl.BlockSpec(memory_space=pltpu.VMEM)] * len(operands),
        out_specs=jax.tree.map(lambda _: pl.BlockSpec(memory_space=pltpu.VMEM), out),
        scratch_shapes=scratch,
        cost_estimate=pl.CostEstimate(flops=flops, bytes_accessed=0, transcendentals=0),
        name=name,
    )(*operands)


def chunk_of(slots):
    for parts in range(1, slots + 1):
        if slots % (8 * parts) == 0 and slots // parts <= 256:
            return slots // parts
    return slots


def on_device(embeddings, cluster_ids, cluster_sizes):
    devices = lax.axis_size("blk")
    rows, width = embeddings.shape
    clusters = cluster_sizes.shape[0]
    bins = devices // CORES
    cap = bin_capacity(rows, devices, clusters)
    slots = bins * cap
    chunk = chunk_of(slots)
    lanes = [[CORES * b + core for b in range(bins)] for core in range(CORES)]
    ids = cluster_ids.reshape(1, rows)
    sizes = cluster_sizes.reshape(1, clusters)

    def shape(*dims, dtype=F32):
        return jax.ShapeDtypeStruct(dims, dtype)

    send, place, of_bin = call(
        functools.partial(pack_kernel, devices, cap),
        (shape(slots, width, dtype=BF16), shape(1, rows), shape(1, clusters)),
        (embeddings, ids, sizes),
        scratch=[pltpu.VMEM((clusters, LANES), F32), pltpu.VMEM((clusters, LANES), F32)],
        name="pack",
    )
    mine = lax.all_to_all(
        send.reshape(bins, cap, width), "blk", 0, 0, tiled=True, axis_index_groups=lanes
    ).reshape(slots, width)
    other = lax.ppermute(mine, "blk", [(i, i ^ 1) for i in range(devices)])
    sums, label_row, label_col = call(
        functools.partial(own_kernel, devices, cap, chunk),
        (shape(2, slots), shape(1, slots), shape(slots, LANES)),
        (mine, sizes, of_bin),
        flops=2 * slots * slots * width,
        name="own",
    )
    out = call(
        functools.partial(mate_kernel, bins, cap, chunk),
        shape(bins, 2, LANES),
        (other, mine, sums, label_row, label_col),
        flops=2 * slots * slots * width,
        name="mate",
    )
    back = lax.all_to_all(out, "blk", 0, 0, tiled=True, axis_index_groups=lanes)
    log_density, centrality = call(
        functools.partial(finish_kernel, bins, cap),
        (shape(1, rows), shape(1, rows)),
        (back, place, ids, sizes),
        name="finish",
    )
    return log_density.reshape(rows), centrality.reshape(rows)


def solution(mesh):
    in_specs = (P(("groups", "blk"), None), P(("groups", "blk")), P("groups"))
    out_specs = (P(("groups", "blk")), P(("groups", "blk")))
    return jax.shard_map(
        on_device, mesh=mesh, in_specs=in_specs, out_specs=out_specs, check_vma=False
    )
```

```python
import functools

import jax
import jax.numpy as jnp
from jax import lax
from jax.experimental import pallas as pl
from jax.experimental.pallas import tpu as pltpu
from jax.sharding import PartitionSpec as P

SOFTMAX_TEMP = 0.1
EPSILON = 1e-06
LANES = 128
CORES = 2
F32 = jnp.float32
BF16 = jnp.bfloat16
FAR = 4096.0
VMEM_LIMIT = 24 * 1024 * 1024


def iota(shape, dim):
    return lax.broadcasted_iota(jnp.int32, shape, dim)


def pick(mask, values, axis):
    return jnp.sum(jnp.where(mask, values, 0.0), axis=axis, keepdims=True)


def one_hot(mask):
    return jnp.where(mask, 1.0, 0.0).astype(BF16)


def matmul(a, b):
    return jnp.dot(a, b, preferred_element_type=F32)


def bin_capacity(rows_dev, devices, clusters):
    total = rows_dev * devices
    largest, fewest = total * 5 // 32, total // 512
    bins = devices // CORES
    heaviest = -(-largest // devices)
    first = devices * (heaviest - 1) + 1
    bound = heaviest
    for k in range(bins + 1, clusters + 1):
        rest = total - first - fewest * (clusters - k)
        for weight in range(1, heaviest + 1):
            least = max(devices * (weight - 1) + 1, fewest)
            if (k - 1) * least > rest:
                break
            others = (rest - least + (devices - 1) * (k - 2)) // devices
            bound = max(bound, others // (bins - 1) + weight)
    return -(-bound // 8) * 8


def held(start, size, device, devices):
    last = jnp.floor((start + size - device + (devices - 1)) * (1.0 / devices))
    return last - jnp.floor((start - device + (devices - 1)) * (1.0 / devices))


def pack_kernel(devices, cap, emb, ids, sizes, send, place, bins_out, weights, picks):
    rows, width = emb.shape
    clusters = sizes.shape[0]
    bins = devices // CORES
    me = lax.axis_index("blk").astype(F32)
    values = emb[...].astype(F32)
    scale = lax.rsqrt(jnp.mean(values * values, axis=1, keepdims=True) + EPSILON)
    unit = (values * (scale * width ** (-0.5))).astype(BF16)

    size = sizes[...].reshape(1, clusters).astype(F32)
    down, across = iota((clusters, clusters), 0), iota((clusters, clusters), 1)
    size_col = pick(down == across, size, 1)
    start = pick(down < across, size_col, 0)
    weight = jnp.floor((size + (devices - 1)) * (1.0 / devices))
    weight_col = jnp.floor((size_col + (devices - 1)) * (1.0 / devices))
    key = weight * clusters - across[:1].astype(F32)
    key_col = weight_col * clusters - down[:, :1].astype(F32)
    rank = pick(key_col > key, 1.0, 0)
    ranked = rank == down.astype(F32)
    weights[...] = jnp.broadcast_to(pick(ranked, weight, 1), weights.shape) * bins

    bin_id = iota((bins, LANES), 0).astype(F32)
    load = weights[:bins, :] + bin_id
    picks[:bins, :] = bin_id
    for t in range(bins, clusters):
        least = jnp.min(load, axis=0, keepdims=True)
        picks[t : t + 1, :] = least
        load = jnp.where(load == least, load + weights[t : t + 1, :], load)
    chosen = picks[...]
    chosen = (chosen - jnp.floor(chosen * (1.0 / bins)) * bins)[:, :clusters]
    of_bin = pick(ranked, chosen, 0)
    bins_out[...] = of_bin
    of_bin_col = pick(down == across, of_bin, 1)
    hold = held(start, size, me, devices)
    offset = pick((of_bin == of_bin_col) & (across < down), hold, 1)
    base = of_bin_col * cap + offset

    member = ids[...].reshape(1, rows) == iota((clusters, rows), 0)
    earlier = one_hot(iota((rows, rows), 0) < iota((rows, rows), 1))
    order = matmul(one_hot(member), earlier)
    target = pick(member, order + base, 0)
    place[...] = target
    slots = bins * cap
    put = one_hot(iota((slots, rows), 0).astype(F32) == target)
    send[...] = matmul(put, unit).astype(BF16)


def pair_sums(left, left_label, right, right_label, chunk):
    density, agreement = 0.0, 0.0
    for at in range(0, left.shape[0], chunk):
        cosine = lax.dot_general(
            left[at : at + chunk, :],
            right,
            (((1,), (1,)), ((), ())),
            preferred_element_type=F32,
        )
        same = left_label[at : at + chunk, :] == right_label
        terms = jnp.where(same, jnp.exp(cosine * (1.0 / SOFTMAX_TEMP)), 0.0)
        density = density + jnp.sum(terms, axis=0, keepdims=True)
        agreement = agreement + jnp.sum(jnp.where(same, cosine, 0.0), axis=0, keepdims=True)
    return density, agreement


def own_kernel(devices, cap, chunk, mine, sizes, bins_in, sums, label_row, label_col):
    clusters = sizes.shape[0]
    bins = devices // CORES
    slots = bins * cap
    me = lax.axis_index("blk")
    core = lax.rem(me, CORES)
    chip = ((me - core) // CORES).astype(F32)
    size = sizes[...].reshape(1, clusters).astype(F32)
    down, across = iota((clusters, clusters), 0), iota((clusters, clusters), 1)
    size_col = pick(down == across, size, 1)
    start = pick(down < across, size_col, 0)
    inside = bins_in[...] == chip
    inside_col = pick((down == across) & inside, 1.0, 1) > 0.0

    def row_labels(parity):
        start_col = pick(across < down, size, 1)
        source = (iota((clusters, bins), 1) * CORES + parity).astype(F32)
        hold = held(start_col, size_col, source, devices).astype(BF16)
        upto = one_hot((across <= down) & inside)
        ends = jnp.where(inside_col, matmul(upto, hold), FAR).astype(BF16)
        low = iota((bins, slots), 0) * cap
        spot = iota((bins, slots), 1)
        block = (spot >= low) & (spot < low + cap)
        slot = pick(block, (spot - low).astype(F32), 0)
        return pick(matmul(ends, one_hot(block)) <= slot, 1.0, 0)

    def col_labels(parity):
        source = (iota((bins, clusters), 0) * CORES + parity).astype(F32)
        hold = held(start, size, source, devices).astype(BF16)
        upto = one_hot((down <= across) & inside_col)
        ends = jnp.where(inside, matmul(hold, upto), FAR).astype(BF16)
        low = iota((slots, bins), 1) * cap
        spot = iota((slots, bins), 0)
        block = (spot >= low) & (spot < low + cap)
        slot = pick(block, (spot - low).astype(F32), 1)
        return pick(matmul(one_hot(block), ends) <= slot, 1.0, 1)

    label = row_labels(core)
    label_row[...] = label
    label_col[...] = jnp.broadcast_to(col_labels(CORES - 1 - core), label_col.shape)
    density, agreement = pair_sums(mine, col_labels(core), mine[...], label, chunk)
    sums[0:1, :] = density
    sums[1:2, :] = agreement


def mate_kernel(bins, cap, chunk, other, mine, sums, label_row, label_col, out):
    density, agreement = pair_sums(other, label_col[:, :1], mine[...], label_row[...], chunk)
    density = density + sums[0:1, :]
    agreement = agreement + sums[1:2, :]
    out[...] = jnp.zeros(out.shape, F32)
    for b in range(bins):
        out[b, 0:1, :cap] = density[:, b * cap : (b + 1) * cap]
        out[b, 1:2, :cap] = agreement[:, b * cap : (b + 1) * cap]


def finish_kernel(bins, cap, back, place, ids, sizes, log_density, centrality):
    rows = ids.shape[0]
    clusters = sizes.shape[0]
    size = sizes[...].reshape(1, clusters).astype(F32)
    size_col = pick(iota((clusters, clusters), 0) == iota((clusters, clusters), 1), size, 1)
    size_row = pick(ids[...].reshape(1, rows) == iota((clusters, rows), 0), size_col, 0)
    target = place[...]
    low = (iota((bins, rows), 0) * cap).astype(F32)
    here = (target >= low) & (target < low + cap)
    slot = pick(here, target - low, 0)
    lane = one_hot(iota((LANES, rows), 0).astype(F32) == slot)

    def fetch(values):
        high = values.astype(BF16)
        left = values - high.astype(F32)
        mid = left.astype(BF16)
        low_part = (left - mid.astype(F32)).astype(BF16)
        found = (matmul(low_part, lane) + matmul(mid, lane)) + matmul(high, lane)
        return pick(here, found, 0)

    log_density[...] = jnp.log(fetch(back[:, 0, :]) / size_row).reshape(rows)
    centrality[...] = (fetch(back[:, 1, :]) / size_row).reshape(rows)


def call(kernel, out, operands, scratch=(), flops=0, name=None):
    return pl.pallas_call(
        kernel,
        out_shape=out,
        in_specs=[pl.BlockSpec(memory_space=pltpu.VMEM)] * len(operands),
        out_specs=jax.tree.map(lambda _: pl.BlockSpec(memory_space=pltpu.VMEM), out),
        scratch_shapes=scratch,
        cost_estimate=pl.CostEstimate(flops=flops, bytes_accessed=0, transcendentals=0),
        compiler_params=pltpu.CompilerParams(vmem_limit_bytes=VMEM_LIMIT),
        name=name,
    )(*operands)


def chunk_of(slots):
    for parts in range(1, slots + 1):
        if slots % (8 * parts) == 0 and slots // parts <= 256:
            return slots // parts
    return slots


def on_device(embeddings, cluster_ids, cluster_sizes):
    devices = lax.axis_size("blk")
    rows, width = embeddings.shape
    clusters = cluster_sizes.shape[0]
    bins = devices // CORES
    cap = bin_capacity(rows, devices, clusters)
    slots = bins * cap
    chunk = chunk_of(slots)
    lanes = [[CORES * b + core for b in range(bins)] for core in range(CORES)]
    ids, sizes = cluster_ids, cluster_sizes

    def shape(*dims, dtype=F32):
        return jax.ShapeDtypeStruct(dims, dtype)

    send, place, of_bin = call(
        functools.partial(pack_kernel, devices, cap),
        (shape(slots, width, dtype=BF16), shape(1, rows), shape(1, clusters)),
        (embeddings, ids, sizes),
        scratch=[pltpu.VMEM((clusters, LANES), F32), pltpu.VMEM((clusters, LANES), F32)],
        name="pack",
    )
    mine = lax.all_to_all(
        send.reshape(bins, cap, width), "blk", 0, 0, tiled=True, axis_index_groups=lanes
    ).reshape(slots, width)
    other = lax.ppermute(mine, "blk", [(i, i ^ 1) for i in range(devices)])
    sums, label_row, label_col = call(
        functools.partial(own_kernel, devices, cap, chunk),
        (shape(2, slots), shape(1, slots), shape(slots, LANES)),
        (mine, sizes, of_bin),
        flops=2 * slots * slots * width,
        name="own",
    )
    out = call(
        functools.partial(mate_kernel, bins, cap, chunk),
        shape(bins, 2, LANES),
        (other, mine, sums, label_row, label_col),
        flops=2 * slots * slots * width,
        name="mate",
    )
    back = lax.all_to_all(out, "blk", 0, 0, tiled=True, axis_index_groups=lanes)
    log_density, centrality = call(
        functools.partial(finish_kernel, bins, cap),
        (shape(rows), shape(rows)),
        (back, place, ids, sizes),
        name="finish",
    )
    return log_density, centrality


def solution(mesh):
    in_specs = (P(("groups", "blk"), None), P(("groups", "blk")), P("groups"))
    out_specs = (P(("groups", "blk")), P(("groups", "blk")))
    return jax.shard_map(
        on_device, mesh=mesh, in_specs=in_specs, out_specs=out_specs, check_vma=False
    )
```
